32 devices in a mesh: filt: 4 (over y, x), dom: 8 (over z, core).
Axes of the slice: x: 2, y: 2, z: 4, core: 2. Of those that a mesh axis runs over, the one named last changes fastest.
Arguments:
- log_weights: float32 [524288], P(('filt', 'dom')), parts along dimension 0, may hold values from -20 to 250, as said below
- bins: int32 [524288], P(('filt', 'dom')), parts along dimension 0, may hold values from 0 to 4095
- states: bfloat16 [128, 524288], P(None, ('filt', 'dom')), parts along dimension 1, may hold values from -6 to 6
Outputs:
- cumulative: float32 [16384], P(('filt', 'dom')), parts along dimension 0
- bin_means: float32 [128, 16384], P(None, ('filt', 'dom')), parts along dimension 1
- particle_weights: float32 [524288], P(('filt', 'dom')), parts along dimension 0
The draws below stay inside these ranges and needn't reach their ends.
There are 4 independent parts, one for each index of `filt`. The reference program is written for one: setup_inputs(seed, part) draws one part's arguments, and reference() takes and returns one part's arrays. A program takes and returns all parts, laid end to end along the dimension named above; each array names one. Nothing has to cross between parts.
Inputs may be any that keep to these rules, and one draw needn't show every extreme that they name: `log_weights`: finite log-weights.
All inputs are finite; a program needn't handle non-finite values.
Results may differ from the reference program's by a relative error of at most 0.00051.
Values sent between devices are 32-bit elements; how exact they have to be, the bound alone decides.
No kernel may reach another device: no remote copies, remote signals or barrier semaphores. Data moves between devices by JAX's collectives and lax.ppermute only.
A program may use at most 64 MiB of HBM per device.

```python
import math
import jax
import jax.numpy as jnp
import numpy as np
from jax import lax

BINS = 4096
STATE = 128
P_DEV = 16384
PARTICLES = 131072
N_DOM = 8


def draw_log_weights(key, part):
    key_offset, key_noise = jax.random.split(jax.random.fold_in(key, 7))
    groups = PARTICLES // P_DEV
    offsets = jax.random.uniform(key_offset, (groups,), jnp.float32, -3.0, 3.0)
    noise = jnp.clip(1.5 * jax.random.normal(key_noise, (groups, P_DEV), jnp.float32), -8.0, 8.0)
    return (offsets[:, None] + noise).reshape(PARTICLES).astype(jnp.float32)


def set_ends(entries, stream_key, least, top_value):
    dims = entries.shape
    spot = [jax.random.randint(jax.random.fold_in(stream_key, axis), (), 0, dims[axis]) for axis in range(len(dims))]
    entries = entries.at[tuple(spot)].set(least)
    longest = dims.index(max(dims))
    spot[longest] = (spot[longest] + 1) % dims[longest]
    return entries.at[tuple(spot)].set(top_value)


def level_of(rng, dims, cuts, smallest, largest):
    gain = 1.0
    for axis_at, blocks in cuts:
        heights = jax.random.uniform(jax.random.fold_in(jax.random.fold_in(rng, 6), axis_at), (blocks,), jnp.float32, smallest / len(cuts), largest / len(cuts))
        gain = gain * jnp.repeat(jnp.exp(heights), dims[axis_at] // blocks).reshape((-1,) + (1,) * (len(dims) - 1 - axis_at))
    return gain


def rank_bounds(count, slope):
    weights = [(1 << 20) // math.isqrt(grade ** slope) + 1 for grade in range(1, count + 1)]
    scale = 1 + sum(weights) // (1 << 30)
    return np.cumsum(np.array([max(1, weight // scale) for weight in weights]))


def ranked(key, extent, amount, lean):
    table = rank_bounds(amount, lean)
    pick = jax.random.randint(jax.random.fold_in(key, 1), extent, 0, int(table[amount - 1]))
    rank = jnp.searchsorted(jnp.asarray(table, jnp.int32), pick, side="right")
    return jax.random.permutation(jax.random.fold_in(key, 2), amount)[rank].astype(jnp.int32)


def scatter_about(stream_key, dims, scale, limit, pieces=(), held_as=jnp.bfloat16):
    level = level_of(stream_key, dims, pieces, -0.22, 0.18) if pieces else 1.0
    entries = jax.random.normal(stream_key, dims, jnp.float32) * scale * level
    return jnp.minimum(jnp.maximum(entries, -limit), limit).astype(held_as)


def setup_inputs(seed: int = 0, part: int = 0) -> dict:
    key_of = jax.random.split(jax.random.key(seed), 4)
    part_splits = jax.random.split(jax.random.fold_in(key_of[3], part), 4)
    log_weights = draw_log_weights(jax.random.fold_in(jax.random.fold_in(key_of[3], part), 71), part)
    bins = set_ends(ranked(part_splits[1], (PARTICLES,), BINS, 2), jax.random.fold_in(part_splits[1], 3), 0, BINS - 1).astype(jnp.int32)
    states = scatter_about(part_splits[2], (STATE, PARTICLES), 1.0, 6.0, ((1, 8),))
    return dict(log_weights=log_weights, bins=bins, states=states)


floor_value = -1.0e4


def group_pairs(group_weights, group_bins, group_states):
    width = min(P_DEV, 1024)
    blocks = P_DEV // width
    labels = lax.iota(jnp.int32, BINS)

    def top_step(index, carry):
        start = (index * width).astype(jnp.int32)
        row_weights = lax.dynamic_slice_in_dim(group_weights, start, width)
        row_bins = lax.dynamic_slice_in_dim(group_bins, start, width)
        member = row_bins[:, None] == labels[None, :]
        return jnp.maximum(carry, jnp.max(jnp.where(member, row_weights[:, None], floor_value), axis=0))

    bin_top = lax.fori_loop(0, blocks, top_step, jnp.full((BINS,), floor_value, jnp.float32))

    def sum_step(index, carry):
        totals, sums = carry
        start = (index * width).astype(jnp.int32)
        row_weights = lax.dynamic_slice_in_dim(group_weights, start, width)
        row_bins = lax.dynamic_slice_in_dim(group_bins, start, width)
        row_states = lax.dynamic_slice_in_dim(group_states, start, width, 1).astype(jnp.float32)
        member = row_bins[:, None] == labels[None, :]
        own_top = jnp.sum(jnp.where(member, bin_top[None, :], jnp.float32(0.0)), axis=1)
        scaled = jnp.exp(row_weights - own_top).astype(jnp.bfloat16).astype(jnp.float32)
        spread = jnp.where(member, scaled[:, None], jnp.float32(0.0))
        totals = totals + jnp.sum(spread, axis=0)
        sums = sums + jnp.dot(row_states, spread, precision=lax.Precision.HIGHEST, preferred_element_type=jnp.float32)
        return totals, sums

    start_pair = (jnp.zeros((BINS,), jnp.float32), jnp.zeros((STATE, BINS), jnp.float32))
    totals, sums = lax.fori_loop(0, blocks, sum_step, start_pair)
    return bin_top, totals, sums


def reference(log_weights, bins, states):
    def one_group(group):
        start = (group * P_DEV).astype(jnp.int32)
        return group_pairs(lax.dynamic_slice_in_dim(log_weights, start, P_DEV),
                           lax.dynamic_slice_in_dim(bins, start, P_DEV),
                           lax.dynamic_slice_in_dim(states, start, P_DEV, 1))

    local_top, local_mass, local_sums = lax.map(one_group, jnp.arange(N_DOM, dtype=jnp.int32))
    bin_top = jnp.max(local_top, axis=0)
    factor = jnp.exp(local_top - bin_top[None, :])
    bin_mass = jnp.sum(local_mass * factor, axis=0)
    bin_sums = jnp.sum(local_sums * factor[:, None, :], axis=0)
    top = jnp.max(bin_top)
    share = bin_mass * jnp.exp(bin_top - top)
    total = jnp.sum(share)
    cumulative = jnp.cumsum(share) / total
    bin_means = bin_sums / jnp.maximum(bin_mass, 1.0)[None, :]
    particle_weights = (P_DEV * N_DOM) * jnp.exp(log_weights - top) / total
    return cumulative, bin_means, particle_weights
```

```python
import functools

import jax
import jax.numpy as jnp
from jax import lax
from jax.experimental import pallas as pl
from jax.experimental.pallas import tpu as pltpu
from jax.sharding import PartitionSpec as P

BINS = 4096
LANES = 128
QUARTERS = 4
SPAN = BINS // QUARTERS
PIECE = 256

floor_value = -10000.0
far = -1.0e30


def local_kernel(groups, lw_ref, bins_ref, st_ref, out_ref, peak_ref, top_ref, w_ref, rest_ref, quarter_ref,
                 left0, right0, left1, right1, acc_ref):
    rows = lw_ref.shape[0]
    states = st_ref.shape[0]
    highs = BINS // LANES
    subs = LANES // 8
    peak_ref[...] = jnp.full(peak_ref.shape, far, jnp.float32)
    label = lax.broadcasted_iota(jnp.int32, (subs, 8, LANES), 0) * 8 + lax.broadcasted_iota(jnp.int32, (subs, 8, LANES), 1)

    def peak_step(index, carry):
        weights, highs_of, gates = [], [], []
        for half in range(2):
            row = index * 2 + half
            weights.append(jnp.broadcast_to(lw_ref[pl.ds(row, 1), :], (8, LANES)))
            row_bins = jnp.broadcast_to(bins_ref[pl.ds(row, 1), :], (8, LANES))
            highs_of.append(row_bins >> 7)
            gates.append(jnp.where(label == (row_bins & 127)[None], jnp.float32(0.0), jnp.float32(far)))
        for high in range(highs):
            parts = [gates[half] + jnp.where(highs_of[half] == high, weights[half], far)[None] for half in range(2)]
            peak_ref[high] = jnp.maximum(peak_ref[high], jnp.maximum(parts[0], parts[1]))
        return carry

    lax.fori_loop(0, rows // 2, peak_step, 0)
    for high in range(highs):
        table = peak_ref[high].reshape(LANES, LANES)
        top_ref[high:high + 1, :] = jnp.maximum(jnp.max(table.T, axis=0, keepdims=True), floor_value)

    own_bins = bins_ref[...]
    low = own_bins & 127
    high_of = own_bins >> 7
    own = jnp.zeros((rows, LANES), jnp.float32)
    for high in range(highs):
        line = jnp.broadcast_to(top_ref[high:high + 1, :], (rows, LANES))
        own = jnp.where(high_of == high, jnp.take_along_axis(line, low, axis=1, mode="promise_in_bounds"), own)
    w_ref[...] = jnp.exp(lw_ref[...] - own).astype(jnp.bfloat16).astype(jnp.float32)
    rest_ref[...] = (own_bins & (SPAN - 1)).astype(jnp.float32)
    quarter_ref[...] = (own_bins >> 10).astype(jnp.float32)

    acc_ref[...] = jnp.zeros(acc_ref.shape, jnp.float32)
    block_rows = left0.shape[1] // LANES
    blocks = rows // block_rows
    tall = PIECE // 16
    count16 = lax.broadcasted_iota(jnp.int32, (tall, 16, LANES), 0) * 16 + lax.broadcasted_iota(jnp.int32, (tall, 16, LANES), 1)
    count16 = count16.astype(jnp.float32).astype(jnp.bfloat16)
    line16 = lax.broadcasted_iota(jnp.int32, (16, LANES), 0).astype(jnp.float32).astype(jnp.bfloat16)
    zero = jnp.zeros((), jnp.bfloat16)

    def build(block, left, right):
        for step in range(block_rows):
            row = block * block_rows + step
            cols = slice(step * LANES, (step + 1) * LANES)
            weight = jnp.broadcast_to(w_ref[pl.ds(row, 1), :], (16, LANES)).astype(jnp.bfloat16)
            rest = jnp.broadcast_to(rest_ref[pl.ds(row, 1), :], (16, LANES))
            quarter = jnp.broadcast_to(quarter_ref[pl.ds(row, 1), :], (16, LANES)).astype(jnp.bfloat16)
            for piece in range(SPAN // PIECE):
                shifted = (rest - float(piece * PIECE)).astype(jnp.bfloat16)
                spread = jnp.where(count16 == shifted[None], weight[None], zero)
                right[piece * PIECE:(piece + 1) * PIECE, cols] = spread.reshape(PIECE, LANES)
            state = st_ref[:, pl.ds(pl.multiple_of(row * LANES, LANES), LANES)].reshape(states // 16, 16, LANES)
            for part in range(QUARTERS):
                kept = jnp.where((quarter == jnp.bfloat16(part))[None], state, zero)
                left[part * states:(part + 1) * states, cols] = kept.reshape(states, LANES)
            left[QUARTERS * states:, cols] = jnp.where(line16 == quarter, jnp.ones((), jnp.bfloat16), zero)

    def gather_in(left, right):
        acc_ref[...] += lax.dot_general(left[...], right[...], (((1,), (1,)), ((), ())), preferred_element_type=jnp.float32)

    build(0, left0, right0)

    def pair_step(index, carry):
        build(index * 2 + 1, left1, right1)
        gather_in(left0, right0)
        build(jnp.minimum(index * 2 + 2, blocks - 1), left0, right0)
        gather_in(left1, right1)
        return carry

    lax.fori_loop(0, blocks // 2, pair_step, 0)

    owned = BINS // groups
    device_top = jnp.max(jnp.max(top_ref[...], axis=1, keepdims=True), axis=0, keepdims=True)
    lane = lax.broadcasted_iota(jnp.int32, (1, LANES), 1)
    masses = jnp.zeros((1, LANES), jnp.float32)
    for group in range(groups):
        first = group * owned
        part, offset = first // SPAN, first % SPAN
        out_ref[group, 0:states, :] = acc_ref[part * states:(part + 1) * states, offset:offset + owned]
        mass = acc_ref[QUARTERS * states + part:QUARTERS * states + part + 1, offset:offset + owned]
        out_ref[group, states:states + 1, :] = mass
        subtotal = jnp.zeros((1, LANES), jnp.float32)
        for tile in range(owned // LANES):
            span = slice(tile * LANES, (tile + 1) * LANES)
            line = top_ref[first // LANES + tile:first // LANES + tile + 1, :]
            out_ref[group, states + 1:states + 2, span] = line
            subtotal = subtotal + mass[:, span] * jnp.exp(line - device_top)
        masses = jnp.where(lane == group, jnp.sum(subtotal, axis=1, keepdims=True), masses)
    for group in range(groups):
        out_ref[group, states + 2:states + 8, :] = jnp.zeros((6, owned), jnp.float32)
        out_ref[group, states + 2:states + 3, 0:LANES] = masses
        out_ref[group, states + 3:states + 4, 0:LANES] = jnp.broadcast_to(device_top, (1, LANES))


def local_pairs(log_weights, bins, states, groups):
    count = log_weights.shape[0]
    rows = count // LANES
    width = states.shape[0]
    block = min(1024, count // 2)
    owned = BINS // groups
    tall = QUARTERS * width + 16
    return pl.pallas_call(
        functools.partial(local_kernel, groups),
        out_shape=jax.ShapeDtypeStruct((groups, width + 8, owned), jnp.float32),
        in_specs=[pl.BlockSpec(memory_space=pltpu.VMEM)] * 3,
        out_specs=pl.BlockSpec(memory_space=pltpu.VMEM),
        scratch_shapes=[
            pltpu.VMEM((BINS // LANES, LANES // 8, 8, LANES), jnp.float32),
            pltpu.VMEM((BINS // LANES, LANES), jnp.float32),
            pltpu.VMEM((rows, LANES), jnp.float32),
            pltpu.VMEM((rows, LANES), jnp.float32),
            pltpu.VMEM((rows, LANES), jnp.float32),
            pltpu.VMEM((tall, block), jnp.bfloat16),
            pltpu.VMEM((SPAN, block), jnp.bfloat16),
            pltpu.VMEM((tall, block), jnp.bfloat16),
            pltpu.VMEM((SPAN, block), jnp.bfloat16),
            pltpu.VMEM((tall, SPAN), jnp.float32),
        ],
        name="local_pairs",
    )(log_weights.reshape(rows, LANES), bins.reshape(rows, LANES), states)


def body(log_weights, bins, states):
    groups = lax.axis_size("dom")
    width = states.shape[0]
    packed = local_pairs(log_weights, bins, states, groups)
    packed = lax.all_to_all(packed, "dom", split_axis=0, concat_axis=0, tiled=True)
    top_pieces = packed[:, width + 1, :]
    owned_top = jnp.max(top_pieces, axis=0)
    factor = jnp.exp(top_pieces - owned_top[None, :])
    owned_mass = jnp.sum(packed[:, width, :] * factor, axis=0)
    owned_sums = jnp.sum(packed[:, :width, :] * factor[:, None, :], axis=0)
    bin_means = owned_sums / jnp.maximum(owned_mass, 1.0)[None, :]
    group_masses = packed[:, width + 2, :groups]
    group_tops = packed[:, width + 3, 0]
    top = jnp.max(group_tops)
    scaled_masses = jnp.sum(group_masses * jnp.exp(group_tops - top)[:, None], axis=0)
    total = jnp.sum(scaled_masses)
    lower = lax.iota(jnp.int32, groups) < lax.axis_index("dom")
    before = jnp.sum(jnp.where(lower, scaled_masses, jnp.float32(0.0)))
    share = owned_mass * jnp.exp(owned_top - top)
    cumulative = (before + jnp.cumsum(share)) / total
    whole_count = log_weights.shape[0] * groups
    particle_weights = whole_count * jnp.exp(log_weights - top) / total
    return (cumulative, bin_means, particle_weights)


def solution(mesh):
    placed = (P(("filt", "dom")), P(("filt", "dom")), P(None, ("filt", "dom")))
    return jax.shard_map(
        body,
        mesh=mesh,
        in_specs=placed,
        out_specs=(P(("filt", "dom")), P(None, ("filt", "dom")), P(("filt", "dom"))),
        check_vma=False,
    )
```

```python
import functools

import jax
import jax.numpy as jnp
from jax import lax
from jax.experimental import pallas as pl
from jax.experimental.pallas import tpu as pltpu
from jax.sharding import PartitionSpec as P

BINS = 4096
LANES = 128
QUARTERS = 4
SPAN = BINS // QUARTERS
PIECE = 256

floor_value = -10000.0
far = -1.0e30


def matmul_sums(width, bins_ref, st_ref, w_ref, rest_ref, quarter_ref, left0, right0, left1, right1, acc_ref):
    rows = bins_ref.shape[0]
    own_bins = bins_ref[...]
    rest_ref[...] = (own_bins & (SPAN - 1)).astype(jnp.float32)
    quarter_ref[...] = (own_bins >> 10).astype(jnp.float32)
    acc_ref[...] = jnp.zeros(acc_ref.shape, jnp.float32)
    block_rows = left0.shape[1] // LANES
    blocks = rows // block_rows
    tall = PIECE // 16
    count16 = lax.broadcasted_iota(jnp.int32, (tall, 16, LANES), 0) * 16 + lax.broadcasted_iota(jnp.int32, (tall, 16, LANES), 1)
    count16 = count16.astype(jnp.float32).astype(jnp.bfloat16)
    line16 = lax.broadcasted_iota(jnp.int32, (16, LANES), 0).astype(jnp.float32).astype(jnp.bfloat16)
    zero = jnp.zeros((), jnp.bfloat16)
    with_mass = left0.shape[0] > QUARTERS * width

    def build(block, left, right):
        for step in range(block_rows):
            row = block * block_rows + step
            cols = slice(step * LANES, (step + 1) * LANES)
            weight = jnp.broadcast_to(w_ref[pl.ds(row, 1), :], (16, LANES)).astype(jnp.bfloat16)
            rest = jnp.broadcast_to(rest_ref[pl.ds(row, 1), :], (16, LANES))
            quarter = jnp.broadcast_to(quarter_ref[pl.ds(row, 1), :], (16, LANES)).astype(jnp.bfloat16)
            for piece in range(SPAN // PIECE):
                shifted = (rest - float(piece * PIECE)).astype(jnp.bfloat16)
                spread = jnp.where(count16 == shifted[None], weight[None], zero)
                right[piece * PIECE:(piece + 1) * PIECE, cols] = spread.reshape(PIECE, LANES)
            state = st_ref[:, pl.ds(pl.multiple_of(row * LANES, LANES), LANES)].reshape(width // 16, 16, LANES)
            for part in range(QUARTERS):
                kept = jnp.where((quarter == jnp.bfloat16(part))[None], state, zero)
                left[part * width:(part + 1) * width, cols] = kept.reshape(width, LANES)
            if with_mass:
                left[QUARTERS * width:, cols] = jnp.where(line16 == quarter, jnp.ones((), jnp.bfloat16), zero)

    def gather_in(left, right):
        acc_ref[...] += lax.dot_general(left[...], right[...], (((1,), (1,)), ((), ())), preferred_element_type=jnp.float32)

    build(0, left0, right0)

    def pair_step(index, carry):
        build(index * 2 + 1, left1, right1)
        gather_in(left0, right0)
        build(jnp.minimum(index * 2 + 2, blocks - 1), left0, right0)
        gather_in(left1, right1)
        return carry

    lax.fori_loop(0, blocks // 2, pair_step, 0)


def write_sums(width, groups, core, keep_ref, give_ref, acc_ref):
    owned = BINS // groups
    for group in range(groups):
        first = group * owned
        part, offset = first // SPAN, first % SPAN
        side = group % 2

        @pl.when(core == side)
        def _():
            keep_ref[group // 2, 0:width, :] = acc_ref[part * width:(part + 1) * width, offset:offset + owned]

        @pl.when(core != side)
        def _():
            give_ref[group // 2, 0:width, :] = acc_ref[part * width:(part + 1) * width, offset:offset + owned]


def first_kernel(groups, me_ref, lw_ref, bins_ref, st_ref, keep_ref, give_ref, w_ref, peak_ref, top_ref, rest_ref, quarter_ref,
                 left0, right0, left1, right1, acc_ref):
    rows = lw_ref.shape[0]
    width = st_ref.shape[0]
    highs = BINS // LANES
    subs = LANES // 8
    core = me_ref[0] % 2
    peak_ref[...] = jnp.full(peak_ref.shape, far, jnp.float32)
    label = lax.broadcasted_iota(jnp.int32, (subs, 8, LANES), 0) * 8 + lax.broadcasted_iota(jnp.int32, (subs, 8, LANES), 1)

    def peak_step(index, carry):
        weights, highs_of, gates = [], [], []
        for half in range(2):
            row = index * 2 + half
            weights.append(jnp.broadcast_to(lw_ref[pl.ds(row, 1), :], (8, LANES)))
            row_bins = jnp.broadcast_to(bins_ref[pl.ds(row, 1), :], (8, LANES))
            highs_of.append(row_bins >> 7)
            gates.append(jnp.where(label == (row_bins & 127)[None], jnp.float32(0.0), jnp.float32(far)))
        for high in range(highs):
            parts = [gates[half] + jnp.where(highs_of[half] == high, weights[half], far)[None] for half in range(2)]
            peak_ref[high] = jnp.maximum(peak_ref[high], jnp.maximum(parts[0], parts[1]))
        return carry

    lax.fori_loop(0, rows // 2, peak_step, 0)
    for high in range(highs):
        table = peak_ref[high].reshape(LANES, LANES)
        top_ref[high:high + 1, :] = jnp.maximum(jnp.max(table.T, axis=0, keepdims=True), floor_value)

    own_bins = bins_ref[...]
    low = own_bins & 127
    high_of = own_bins >> 7
    own = jnp.zeros((rows, LANES), jnp.float32)
    for high in range(highs):
        line = jnp.broadcast_to(top_ref[high:high + 1, :], (rows, LANES))
        own = jnp.where(high_of == high, jnp.take_along_axis(line, low, axis=1, mode="promise_in_bounds"), own)
    w_ref[...] = jnp.exp(lw_ref[...] - own).astype(jnp.bfloat16).astype(jnp.float32)

    matmul_sums(width, bins_ref, st_ref, w_ref, rest_ref, quarter_ref, left0, right0, left1, right1, acc_ref)
    write_sums(width, groups, core, keep_ref, give_ref, acc_ref)

    owned = BINS // groups
    device_top = jnp.max(jnp.max(top_ref[...], axis=1, keepdims=True), axis=0, keepdims=True)
    lane = lax.broadcasted_iota(jnp.int32, (1, LANES), 1)
    masses = jnp.zeros((1, LANES), jnp.float32)

    def tail(group):
        first = group * owned
        part, offset = first // SPAN, first % SPAN
        mass = acc_ref[QUARTERS * width + part:QUARTERS * width + part + 1, offset:offset + owned]
        line = jnp.concatenate([top_ref[first // LANES + tile:first // LANES + tile + 1, :] for tile in range(owned // LANES)], axis=1)
        return mass, line

    for group in range(groups):
        mass, line = tail(group)
        masses = jnp.where(lane == group, jnp.sum(mass * jnp.exp(line - device_top), axis=1, keepdims=True), masses)
    blank = jnp.zeros((1, owned - LANES), jnp.float32)
    masses = jnp.concatenate([masses, blank], axis=1) if owned > LANES else masses
    spread_top = jnp.broadcast_to(device_top, (1, owned))
    rest_rows = jnp.zeros((4, owned), jnp.float32)
    for group in range(groups):
        mass, line = tail(group)
        block = jnp.concatenate([mass, line, masses, spread_top, rest_rows], axis=0)
        side = group % 2

        @pl.when(core == side)
        def _():
            keep_ref[group // 2, width:width + 8, :] = block

        @pl.when(core != side)
        def _():
            give_ref[group // 2, width:width + 8, :] = block


def second_kernel(groups, me_ref, w_ref, bins_ref, st_ref, order_ref, keep_ref, give_ref, rest_ref, quarter_ref,
                  left0, right0, left1, right1, acc_ref):
    width = st_ref.shape[0]
    matmul_sums(width, bins_ref, st_ref, w_ref, rest_ref, quarter_ref, left0, right0, left1, right1, acc_ref)
    write_sums(width, groups, me_ref[0] % 2, keep_ref, give_ref, acc_ref)


def merge_first(width, me_ref, keep_ref, got_ref, factor_ref, *outs):
    chips = keep_ref.shape[0]
    mine = me_ref[0] // 2
    for shift in range(chips):
        at = (mine + shift) % chips
        tail_a, tail_b = keep_ref[at, width:width + 8, :], got_ref[at, width:width + 8, :]
        best = jnp.maximum(tail_a[1:2], tail_b[1:2])
        fa, fb = jnp.exp(tail_a[1:2] - best), jnp.exp(tail_b[1:2] - best)
        peak = jnp.maximum(tail_a[3:4], tail_b[3:4])
        masses = tail_a[2:3] * jnp.exp(tail_a[3:4] - peak) + tail_b[2:3] * jnp.exp(tail_b[3:4] - peak)
        outs[shift][0:width, :] = keep_ref[at, 0:width, :] * fa + got_ref[at, 0:width, :] * fb
        mass = tail_a[0:1] * fa + tail_b[0:1] * fb
        outs[shift][width:width + 8, :] = jnp.concatenate([mass, best, masses, peak, tail_a[4:8]], axis=0)
        factor_ref[shift, :, :] = jnp.concatenate([fa, fb, tail_a[0:6] * 0.0], axis=0)


def merge_second(me_ref, factor_ref, keep_ref, got_ref, *outs):
    chips = keep_ref.shape[0]
    mine = me_ref[0] // 2
    for shift in range(chips):
        at = (mine + shift) % chips
        outs[shift][...] = keep_ref[at] * factor_ref[shift, 0:1, :] + got_ref[at] * factor_ref[shift, 1:2, :]


def final_kernel(width, count, me_ref, lw_ref, *refs):
    chips = (len(refs) - 3) // 2
    firsts, seconds = refs[:chips], refs[chips:2 * chips]
    cumulative_ref, means_ref, particle_ref = refs[2 * chips:]
    tails = [first[width:width + 8, :] for first in firsts]
    best = functools.reduce(jnp.maximum, [tail[1:2] for tail in tails])
    peak = functools.reduce(jnp.maximum, [tail[3:4] for tail in tails])
    factors = [jnp.exp(tail[1:2] - best) for tail in tails]
    mass = sum(tail[0:1] * factor for tail, factor in zip(tails, factors))
    masses = sum(tail[2:3] * jnp.exp(tail[3:4] - peak) for tail in tails)
    owned = mass.shape[1]
    lane = lax.broadcasted_iota(jnp.int32, (1, owned), 1)
    total = jnp.sum(masses, axis=1, keepdims=True)
    before = jnp.sum(jnp.where(lane < me_ref[0], masses, 0.0), axis=1, keepdims=True)
    share = mass * jnp.exp(best - peak)
    upper = (lax.broadcasted_iota(jnp.int32, (owned, owned), 0) <= lax.broadcasted_iota(jnp.int32, (owned, owned), 1))
    running = jnp.dot(jnp.broadcast_to(share, (8, owned)), upper.astype(jnp.float32), precision=lax.Precision.HIGHEST,
                      preferred_element_type=jnp.float32)[0:1]
    cumulative_ref[...] = (before + running) / total
    floored = jnp.maximum(mass, 1.0)
    means_ref[0:width, :] = sum(first[0:width, :] * factor for first, factor in zip(firsts, factors)) / floored
    means_ref[width:2 * width, :] = sum(second[...] * factor for second, factor in zip(seconds, factors)) / floored
    particle_ref[...] = count * jnp.exp(lw_ref[...] - peak[:, 0:1]) / total


def body(log_weights, bins, states):
    groups = lax.axis_size("dom")
    chips = groups // 2
    count = log_weights.shape[0]
    rows = count // LANES
    width = states.shape[0] // 2
    block = min(2048, count // 2)
    owned = BINS // groups
    me = lax.axis_index("dom").astype(jnp.int32)[None]
    vmem, smem = pl.BlockSpec(memory_space=pltpu.VMEM), pl.BlockSpec(memory_space=pltpu.SMEM)
    lw2, bins2 = log_weights.reshape(rows, LANES), bins.reshape(rows, LANES)

    def shape(*dims):
        return jax.ShapeDtypeStruct(dims, jnp.float32)

    def matmul_scratch(tall):
        return [
            pltpu.VMEM((rows, LANES), jnp.float32),
            pltpu.VMEM((rows, LANES), jnp.float32),
            pltpu.VMEM((tall, block), jnp.bfloat16),
            pltpu.VMEM((SPAN, block), jnp.bfloat16),
            pltpu.VMEM((tall, block), jnp.bfloat16),
            pltpu.VMEM((SPAN, block), jnp.bfloat16),
            pltpu.VMEM((tall, SPAN), jnp.float32),
        ]

    siblings = [(spot, spot ^ 1) for spot in range(groups)]

    def along(shift):
        return [(spot, (spot + 2 * shift) % groups) for spot in range(groups)]

    keep1, give1, weights = pl.pallas_call(
        functools.partial(first_kernel, groups),
        out_shape=(shape(chips, width + 8, owned), shape(chips, width + 8, owned), shape(rows, LANES)),
        grid=(1,),
        in_specs=[smem, vmem, vmem, pl.BlockSpec((width, count), lambda i: (0, 0))],
        out_specs=[vmem, vmem, vmem],
        scratch_shapes=[
            pltpu.VMEM((BINS // LANES, LANES // 8, 8, LANES), jnp.float32),
            pltpu.VMEM((BINS // LANES, LANES), jnp.float32),
        ] + matmul_scratch(QUARTERS * width + 16),
        name="first_half",
    )(me, lw2, bins2, states)
    got1 = lax.ppermute(give1, "dom", siblings)
    factor, *merged1 = pl.pallas_call(
        functools.partial(merge_first, width),
        out_shape=(shape(chips, 8, owned),) + (shape(width + 8, owned),) * chips,
        in_specs=[smem, vmem, vmem],
        out_specs=[vmem] * (chips + 1),
        name="merge_first",
    )(me, keep1, got1)
    firsts = [merged1[0]]
    for shift in range(1, chips):
        firsts.append(lax.ppermute(merged1[shift], "dom", along(shift)))
    second = pl.pallas_call(
        functools.partial(second_kernel, groups),
        out_shape=(shape(chips, width, owned), shape(chips, width, owned)),
        grid=(1,),
        in_specs=[smem, vmem, vmem, pl.BlockSpec((width, count), lambda i: (1, 0)), pl.BlockSpec(memory_space=pl.ANY)],
        out_specs=[vmem, vmem],
        scratch_shapes=matmul_scratch(QUARTERS * width),
        name="second_half",
    )
    keep2, give2 = second(me, weights, bins2, states, factor)
    got2 = lax.ppermute(give2, "dom", siblings)
    merged2 = pl.pallas_call(
        merge_second,
        out_shape=(shape(width, owned),) * chips,
        in_specs=[smem, vmem, vmem, vmem],
        out_specs=[vmem] * chips,
        name="merge_second",
    )(me, factor, keep2, got2)
    seconds = [merged2[0]] + [lax.ppermute(merged2[shift], "dom", along(shift)) for shift in range(1, chips)]
    cumulative, bin_means, particle_weights = pl.pallas_call(
        functools.partial(final_kernel, width, float(count * groups)),
        out_shape=(shape(1, owned), shape(2 * width, owned), shape(rows, LANES)),
        in_specs=[smem, vmem] + [vmem] * (2 * chips),
        out_specs=[vmem, vmem, vmem],
        name="final_merge",
    )(me, lw2, *firsts, *seconds)
    return (cumulative.reshape(owned), bin_means, particle_weights.reshape(count))


def solution(mesh):
    placed = (P(("filt", "dom")), P(("filt", "dom")), P(None, ("filt", "dom")))
    return jax.shard_map(
        body,
        mesh=mesh,
        in_specs=placed,
        out_specs=(P(("filt", "dom")), P(None, ("filt", "dom")), P(("filt", "dom"))),
        check_vma=False,
    )
```
